128 devices in a mesh: row: 8 (over z, core), col: 16 (over y, x).
Axes of the slice: x: 4, y: 4, z: 4, core: 2. Of those that a mesh axis runs over, the one named last changes fastest.
Arguments:
- factor_wide: float32 [2, 8, 1, 16, 512, 512], P(None, 'row', None, 'col'), may hold values from -1 to 2, as said below
- factor_narrow: bfloat16 [2, 8, 1, 16, 512, 512], P(None, 'row', None, 'col'), may hold values from -1 to 2, as said below
- flags: int32 [2, 8, 1, 16], P(None, 'row', None, 'col'), may hold values from 0 to 1
- forward_solution: float32 [1, 16, 512, 128], P(None, 'col'), may hold values from -0.5 to 0.5
- solution_grad: float32 [1, 16, 512, 128], P(None, 'col'), may hold values from -1.8 to 1.8
Outputs:
- rhs_grad: float32 [2, 8, 512, 128], P(None, 'row')
- factor_grad: float32 [2, 8, 1, 16, 512, 512], P(None, 'row', None, 'col')
The draws below stay inside these ranges and needn't reach their ends.
Inputs may be any that keep to these rules, and one draw needn't show every extreme that they name: `factor_wide`: the diagonal entries of every diagonal tile lie between 1 and 2. `factor_narrow`: the diagonal entries of every diagonal tile lie between 1 and 2.
All inputs are finite; a program needn't handle non-finite values.
Results may differ from the reference program's by a relative error of at most 0.0003.
Values sent between devices are 32-bit elements; how exact they have to be, the bound alone decides.
A program may use at most 64 MiB of HBM per device.

```python
import math
import jax
import jax.numpy as jnp
from jax import lax

TB = 512
NT = 16
R = 128
N_ROW = 8
N_COL = 16


coupling = 3.0


def factor_law(key):
    shape = (NT // N_ROW, N_ROW, NT // N_COL, N_COL, TB, TB)
    spread = jax.random.normal(key, shape, jnp.float32)
    diagonal = jax.random.uniform(jax.random.fold_in(key, 5), shape, jnp.float32, 1.0, 2.0)
    scaled = spread * (coupling / math.sqrt(NT * TB))
    row_shape = (NT // N_ROW, N_ROW, 1, 1, 1, 1)
    col_shape = (1, 1, NT // N_COL, N_COL, 1, 1)
    inner_shape = (1, 1, 1, 1, TB, TB)
    tile_row = lax.broadcasted_iota(jnp.int32, row_shape, 0) * N_ROW + lax.broadcasted_iota(jnp.int32, row_shape, 1)
    tile_col = lax.broadcasted_iota(jnp.int32, col_shape, 2) * N_COL + lax.broadcasted_iota(jnp.int32, col_shape, 3)
    inner_row = lax.broadcasted_iota(jnp.int32, inner_shape, 4)
    inner_col = lax.broadcasted_iota(jnp.int32, inner_shape, 5)
    on_diagonal = (tile_row == tile_col) & (inner_row == inner_col)
    return jnp.where(on_diagonal, diagonal, scaled)


def draw_factor_wide(key, part):
    return factor_law(jax.random.fold_in(key, 11))


def draw_factor_narrow(key, part):
    return factor_law(jax.random.fold_in(key, 23)).astype(jnp.bfloat16)


def with_ends(entries, rng, smallest, high):
    longest = entries.shape.index(max(entries.shape))
    spots = []
    for shift in (0, 1):
        where = [jax.random.randint(jax.random.fold_in(rng, axis), (), 0, length) for axis, length in enumerate(entries.shape)]
        where[longest] = (where[longest] + shift) % entries.shape[longest]
        spots.append(tuple(where))
    return entries.at[spots[0]].set(smallest).at[spots[1]].set(high)


def block_scale(rng, shape, split, low, high):
    loudness = 1.0
    for position, shards_of in split:
        heights = jax.random.uniform(jax.random.fold_in(jax.random.fold_in(rng, 6), position), (shards_of,), jnp.float32, low / len(split), high / len(split))
        loudness = loudness * jnp.repeat(jnp.exp(heights), shape[position] // shards_of).reshape((-1,) + (1,) * (len(shape) - 1 - position))
    return loudness


def normal_values(stream_key, shape, width, most, cuts=(), held_as=jnp.bfloat16):
    drawn = jax.random.normal(stream_key, shape, jnp.float32) * width
    if len(cuts) > 0:
        drawn = block_scale(stream_key, shape, cuts, -0.22, 0.18) * drawn
    return jnp.clip(drawn, min=-most, max=most).astype(held_as)


def setup_inputs(seed: int = 0) -> dict:
    seeds = jax.random.split(jax.random.key(seed), 6)
    factor_wide = draw_factor_wide(jax.random.fold_in(seeds[5], 71), 0)
    factor_narrow = draw_factor_narrow(jax.random.fold_in(seeds[5], 71), 0)
    flags = with_ends(jax.random.randint(seeds[2], (NT // N_ROW, N_ROW, NT // N_COL, N_COL), 0, 2), jax.random.fold_in(seeds[2], 1), 0, 1).astype(jnp.int32)
    forward_solution = normal_values(seeds[3], (NT // N_COL, N_COL, TB, R), R ** -0.5, 0.5, ((1, 16),), jnp.float32)
    solution_grad = normal_values(seeds[4], (NT // N_COL, N_COL, TB, R), 0.3, 1.8, ((1, 16),), jnp.float32)
    return {"factor_wide": factor_wide, "factor_narrow": factor_narrow, "flags": flags, "forward_solution": forward_solution, "solution_grad": solution_grad}


HIGHEST_PRECISION = lax.Precision.HIGHEST

def lower_mask(row_index, col_index, tile_width):
    inner_mask = lax.broadcasted_iota(jnp.int32, (tile_width, tile_width), 0) >= lax.broadcasted_iota(jnp.int32, (tile_width, tile_width), 1)
    return (row_index > col_index) | (row_index == col_index) & inner_mask

def reference(factor_wide, factor_narrow, flags, forward_solution, solution_grad):
    chosen = jnp.where(flags[:, :, :, :, None, None] == 1, factor_narrow.astype(jnp.float32), factor_wide)
    factor_tiles = chosen.reshape(NT, NT, TB, TB)
    solution_tiles = forward_solution.reshape(NT, TB, R)
    target_tiles = solution_grad.reshape(NT, TB, R)
    solved_tiles = [None] * NT
    for target in range(NT - 1, -1, -1):
        right_side = target_tiles[target]
        for source in range(target + 1, NT):
            right_side = right_side - jnp.dot(factor_tiles[source, target].T.astype(jnp.float32), solved_tiles[source].astype(jnp.float32), precision=HIGHEST_PRECISION, preferred_element_type=jnp.float32)
        solved_tiles[target] = lax.linalg.triangular_solve(factor_tiles[target, target], right_side, left_side=True, lower=True, transpose_a=True)
    rhs_grad = jnp.stack(solved_tiles)
    products = -jnp.einsum('akr,blr->abkl', rhs_grad, solution_tiles, precision=HIGHEST_PRECISION)
    tile_index = jnp.arange(NT, dtype=jnp.int32)
    masks = lower_mask(tile_index[:, None, None, None], tile_index[None, :, None, None], TB)
    factor_grad = jnp.where(masks, products, jnp.zeros_like(products))
    return (rhs_grad.reshape(NT // N_ROW, N_ROW, TB, R), factor_grad.reshape(NT // N_ROW, N_ROW, NT // N_COL, N_COL, TB, TB))
```

```python
import functools

import jax
import jax.numpy as jnp
from jax import lax
from jax.experimental import pallas as pl
from jax.experimental.pallas import tpu as pltpu
from jax.sharding import PartitionSpec as P

MESH = pl.DeviceIdType.MESH
F32 = jnp.float32
BF16 = jnp.bfloat16
CHUNKS = 8


def halves(value):
    high = value.astype(BF16)
    return high, (value - high.astype(F32)).astype(BF16)


def mul(a, b):
    return jnp.dot(a, b, preferred_element_type=F32)


def dot3(left, high, low):
    left_high, left_low = halves(left)
    rows = left.shape[0]
    both = mul(jnp.concatenate([left_high, left_low], axis=0), high)
    return both[:rows] + both[rows:] + mul(left_high, low)


def dot_full(left, right):
    left_high, left_low = halves(left)
    right_high, right_low = halves(right)
    return mul(left_high, right_high) + (mul(left_low, right_high) + mul(left_high, right_low))


def kernel(
    sizes,
    flags,
    wide_hbm,
    narrow_hbm,
    x_ref,
    g_ref,
    rhs_hbm,
    grad_hbm,
    wide,
    narrow,
    l_high,
    l_low,
    below,
    w_full,
    w_high,
    w_low,
    v_high,
    v_low,
    g_turned,
    x_high,
    x_low,
    y_buf,
    chain,
    part,
    rhs_out,
    grad_out,
    load_sem,
    store_sem,
    below_send,
    below_recv,
    chain_send,
    chain_recv,
    row_recv,
    x_send,
    y_send,
    part_send,
    part_recv,
):
    n_row, n_col, nx, ny, tile, rhs, chunks = sizes
    n_tiles = 2 * n_row
    width = rhs // chunks
    r = lax.axis_index("row")
    c = lax.axis_index("col")
    x = lax.rem(c, nx)
    y = lax.div(c, nx)
    diag_row = lax.rem(c, n_row)
    diag_slot = lax.div(c, n_row)
    is_diag = r == diag_row

    loads = [
        pltpu.make_async_copy(wide_hbm.at[s], wide.at[s], load_sem.at[s]) for s in range(2)
    ] + [
        pltpu.make_async_copy(narrow_hbm.at[s], narrow.at[s], load_sem.at[2 + s]) for s in range(2)
    ]
    for load in loads:
        load.start()

    barrier = pltpu.get_barrier_semaphore()

    def greet(row, col):
        pl.semaphore_signal(barrier, inc=1, device_id=(row, col), device_id_type=MESH)

    for d in range(1, nx):
        greet(r, y * nx + lax.rem(x + d, nx))
    for d in range(1, ny):
        greet(r, lax.rem(y + d, ny) * nx + x)
    for d in range(1, n_row):
        greet(lax.rem(r + d, n_row), c)
    peers = nx + ny + n_row - 3

    @pl.when(is_diag & (c > 0))
    def _():
        greet(lax.rem(c + n_row - 1, n_row), c - 1)

    @pl.when(is_diag & (c < n_tiles - 1))
    def _():
        greet(lax.rem(c + 1, n_row), c + 1)

    links = jnp.where(c > 0, 1, 0) + jnp.where(c < n_tiles - 1, 1, 0)
    pl.semaphore_wait(barrier, peers + jnp.where(is_diag, links, 0))

    for load in loads:
        load.wait()
    step = min(64, tile)
    for s in range(2):
        from_narrow = flags[s] == 1

        def choose(n, _, s=s, from_narrow=from_narrow):
            rows = pl.ds(pl.multiple_of(n * step, step), step)
            value = jnp.where(from_narrow, narrow[s, rows, :].astype(F32), wide[s, rows, :])
            wide[s, rows, :] = value
            high, low = halves(value)
            l_high[s, rows, :] = high
            l_low[s, rows, :] = low
            return 0

        lax.fori_loop(0, tile // step, choose, 0)

    holds_below = (r == lax.rem(c + 1, n_row)) & (c < n_tiles - 1)
    below_slot = jnp.minimum(lax.div(c + 1, n_row), 1)
    below_copy = pltpu.make_async_remote_copy(
        src_ref=wide.at[below_slot],
        dst_ref=below,
        send_sem=below_send.at[0],
        recv_sem=below_recv.at[0],
        device_id=(diag_row, c),
        device_id_type=MESH,
    )

    @pl.when(holds_below)
    def _():
        below_copy.start()

    turned_x = jnp.transpose(x_ref[...])
    x_high[...], x_low[...] = halves(turned_x)

    half = tile // 2

    def sends_part(row):
        return (row != diag_row) & (row + n_row >= c + 2)

    @pl.when(is_diag)
    def _():
        turned_g = jnp.transpose(g_ref[...])
        for k in range(chunks):
            g_turned[k] = turned_g[k * width : (k + 1) * width]
        for row in range(n_row):

            @pl.when(jnp.logical_not(sends_part(row)))
            def _(row=row):
                part[row] = jnp.zeros(part.shape[1:], F32)

        rows = lax.broadcasted_iota(jnp.int32, (half, half), 0)
        cols = lax.broadcasted_iota(jnp.int32, (half, half), 1)
        for b in range(2):
            w_full[b * half : (b + 1) * half, b * half : (b + 1) * half] = jnp.zeros((half, half), F32)
        blocks = []
        inverses = []
        for b in range(2):
            at = slice(b * half, (b + 1) * half)
            block = wide[diag_slot, at, at]
            on_diag = jnp.where(rows == cols, block, 0.0)
            down = 1.0 / jnp.sum(on_diag, axis=1, keepdims=True)
            across = 1.0 / jnp.sum(on_diag, axis=0, keepdims=True)
            pairs = (rows == cols + 1) & (lax.rem(rows, 2) == 1)
            inverse = jnp.where(rows == cols, down, 0.0) - jnp.where(pairs, block * down * across, 0.0)
            blocks.append(block)
            inverses.append(inverse)
        size = 2
        while size < half:
            mask = (lax.div(rows, 2 * size) == lax.div(cols, 2 * size)) & (
                lax.rem(lax.div(rows, size), 2) > lax.rem(lax.div(cols, size), 2)
            )
            for b in range(2):
                coupling = jnp.where(mask, blocks[b], 0.0)
                product = dot_full(coupling, inverses[b])
                inverses[b] = inverses[b] - dot_full(inverses[b], product)
            size *= 2
        coupling = wide[diag_slot, half:, :half]
        product = dot_full(coupling, inverses[0])
        corner = -dot_full(inverses[1], product)
        w_full[:half, :half] = inverses[0]
        w_full[:half, half:] = jnp.zeros((half, half), F32)
        w_full[half:, :half] = corner
        w_full[half:, half:] = inverses[1]
        high, low = halves(w_full[...])
        w_high[...] = high
        w_low[...] = low

        @pl.when(c < n_tiles - 1)
        def _():
            below_copy.wait_recv()

            def fold(n, _):
                at = pl.ds(pl.multiple_of(n * (tile // 4), tile // 4), tile // 4)
                high, low = halves(dot3(below[at, :], w_high[...], w_low[...]))
                v_high[at, :] = high
                v_low[at, :] = low
                return 0

            lax.fori_loop(0, 4, fold, 0)

    def chain_copy(k):
        return pltpu.make_async_remote_copy(
            src_ref=y_buf.at[diag_slot, k],
            dst_ref=chain.at[k],
            send_sem=chain_send.at[k],
            recv_sem=chain_recv.at[k],
            device_id=(lax.rem(c + n_row - 1, n_row), jnp.maximum(c - 1, 0)),
            device_id_type=MESH,
        )

    def x_copy(s, k, d):
        return pltpu.make_async_remote_copy(
            src_ref=y_buf.at[s, k],
            dst_ref=y_buf.at[s, k],
            send_sem=x_send.at[d, k],
            recv_sem=row_recv.at[s, k],
            device_id=(r, y * nx + lax.rem(x + d, nx)),
            device_id_type=MESH,
        )

    def y_copy(s, k, d):
        return pltpu.make_async_remote_copy(
            src_ref=y_buf.at[s, k],
            dst_ref=y_buf.at[s, k],
            send_sem=y_send.at[s, d, k],
            recv_sem=row_recv.at[s, k],
            device_id=(r, lax.rem(y + d, ny) * nx + x),
            device_id_type=MESH,
        )

    def part_copy(row, k):
        return pltpu.make_async_remote_copy(
            src_ref=part.at[row, k],
            dst_ref=part.at[row, k],
            send_sem=part_send.at[k],
            recv_sem=part_recv.at[row, k],
            device_id=(diag_row, c),
            device_id_type=MESH,
        )

    for s in (1, 0):
        i = r + n_row * s
        is_source = i == c
        in_source_line = lax.div(i, nx) == y
        takes_part = i >= c + 2
        if s == 1:
            sends_now = takes_part & (r != diag_row) & (r < c + 2)
        else:
            sends_now = takes_part

        @pl.when(is_source)
        def _(s=s):
            def solve(k, _):
                for row in range(n_row):

                    @pl.when(sends_part(row))
                    def _(row=row):
                        part_copy(row, k).wait_recv()

                total = g_turned[k]
                for row in range(n_row):
                    total = total - part[row, k]
                base = dot3(total, w_high[...], w_low[...])
                y_buf[s, k] = base

                @pl.when(c < n_tiles - 1)
                def _():
                    chain_copy(k).wait_recv()
                    y_buf[s, k] = base - dot3(chain[k], v_high[...], v_low[...])

                @pl.when(c > 0)
                def _():
                    chain_copy(k).start()

                for d in range(nx - 1, 0, -1):
                    x_copy(s, k, d).start()
                for d in range(ny - 1, 0, -1):
                    y_copy(s, k, d).start()
                return 0

            lax.fori_loop(0, chunks, solve, 0)

        @pl.when(jnp.logical_not(is_source))
        def _(s=s, in_source_line=in_source_line, takes_part=takes_part, sends_now=sends_now):
            def take(k, _):
                x_copy(s, k, 1).wait_recv()

                @pl.when(in_source_line)
                def _():
                    for d in range(ny - 1, 0, -1):
                        y_copy(s, k, d).start()

                @pl.when(takes_part)
                def _():
                    product = dot3(y_buf[s, k], l_high[s], l_low[s])
                    if s == 0:
                        product = product + part[r, k]
                    part[r, k] = product

                @pl.when(sends_now)
                def _():
                    part_copy(r, k).start()

                return 0

            lax.fori_loop(0, chunks, take, 0)

        block = jnp.concatenate([y_buf[s, k] for k in range(chunks)], axis=0)
        rhs_out[s] = jnp.transpose(block)
        quarter = tile // 4

        def outer(n, _, s=s, i=i):
            at = pl.ds(pl.multiple_of(n * quarter, quarter), quarter)
            value = -dot3(rhs_out[s, at, :], x_high[...], x_low[...])
            rows = lax.broadcasted_iota(jnp.int32, (quarter, tile), 0) + n * quarter
            cols = lax.broadcasted_iota(jnp.int32, (quarter, tile), 1)
            keep = (rows + i * tile) >= (cols + c * tile)
            grad_out[s, at, :] = jnp.where(keep, value, 0.0)
            return 0

        lax.fori_loop(0, 4, outer, 0)
        pltpu.make_async_copy(rhs_out.at[s], rhs_hbm.at[s], store_sem.at[s]).start()
        pltpu.make_async_copy(grad_out.at[s], grad_hbm.at[s], store_sem.at[2 + s]).start()

    @pl.when(holds_below)
    def _():
        below_copy.wait_send()

    for s in (1, 0):
        i = r + n_row * s
        in_source_line = lax.div(i, nx) == y
        takes_part = i >= c + 2
        if s == 1:
            sends_now = takes_part & (r != diag_row) & (r < c + 2)
        else:
            sends_now = takes_part

        @pl.when(i == c)
        def _(s=s):
            def ended(k, _):
                @pl.when(c > 0)
                def _():
                    chain_copy(k).wait_send()

                for d in range(1, nx):
                    x_copy(s, k, d).wait_send()
                return 0

            lax.fori_loop(0, chunks, ended, 0)

        @pl.when(in_source_line)
        def _(s=s):
            def ended(k, _):
                for d in range(1, ny):
                    y_copy(s, k, d).wait_send()
                return 0

            lax.fori_loop(0, chunks, ended, 0)

        @pl.when((i != c) & sends_now)
        def _():
            def ended(k, _):
                part_copy(r, k).wait_send()
                return 0

            lax.fori_loop(0, chunks, ended, 0)

        pltpu.make_async_copy(rhs_out.at[s], rhs_hbm.at[s], store_sem.at[s]).wait()
        pltpu.make_async_copy(grad_out.at[s], grad_hbm.at[s], store_sem.at[2 + s]).wait()


def solution(mesh):
    n_row, n_col = mesh.shape["row"], mesh.shape["col"]
    nx = 4 if n_col == 16 else 2
    ny = n_col // nx

    def body(factor_wide, factor_narrow, flags, forward_solution, solution_grad):
        slots, _, _, _, tile, _ = factor_wide.shape
        rhs = forward_solution.shape[-1]
        chunks = CHUNKS
        width = rhs // chunks
        sizes = (n_row, n_col, nx, ny, tile, rhs, chunks)
        vmem = pltpu.VMEM
        dma = pltpu.SemaphoreType.DMA
        rhs_grad, factor_grad = pl.pallas_call(
            functools.partial(kernel, sizes),
            out_shape=(
                jax.ShapeDtypeStruct((slots, tile, rhs), F32),
                jax.ShapeDtypeStruct((slots, tile, tile), F32),
            ),
            in_specs=[
                pl.BlockSpec(memory_space=pltpu.SMEM),
                pl.BlockSpec(memory_space=pl.ANY),
                pl.BlockSpec(memory_space=pl.ANY),
                pl.BlockSpec(memory_space=pltpu.VMEM),
                pl.BlockSpec(memory_space=pltpu.VMEM),
            ],
            out_specs=(
                pl.BlockSpec(memory_space=pl.ANY),
                pl.BlockSpec(memory_space=pl.ANY),
            ),
            scratch_shapes=[
                vmem((slots, tile, tile), F32),
                vmem((slots, tile, tile), BF16),
                vmem((slots, tile, tile), BF16),
                vmem((slots, tile, tile), BF16),
                vmem((tile, tile), F32),
                vmem((tile, tile), F32),
                vmem((tile, tile), BF16),
                vmem((tile, tile), BF16),
                vmem((tile, tile), BF16),
                vmem((tile, tile), BF16),
                vmem((chunks, width, tile), F32),
                vmem((rhs, tile), BF16),
                vmem((rhs, tile), BF16),
                vmem((slots, chunks, width, tile), F32),
                vmem((chunks, width, tile), F32),
                vmem((n_row, chunks, width, tile), F32),
                vmem((slots, tile, rhs), F32),
                vmem((slots, tile, tile), F32),
                dma((4,)),
                dma((4,)),
                dma((1,)),
                dma((1,)),
                dma((chunks,)),
                dma((chunks,)),
                dma((slots, chunks)),
                dma((nx, chunks)),
                dma((slots, ny, chunks)),
                dma((chunks,)),
                dma((n_row, chunks)),
            ],
            compiler_params=pltpu.CompilerParams(collective_id=0, has_side_effects=True),
        )(
            flags.reshape(slots),
            factor_wide.reshape(slots, tile, tile),
            factor_narrow.reshape(slots, tile, tile),
            forward_solution.reshape(tile, rhs),
            solution_grad.reshape(tile, rhs),
        )
        return (
            rhs_grad[:, None],
            factor_grad.reshape(slots, 1, 1, 1, tile, tile),
        )

    placed = (
        P(None, "row", None, "col", None, None),
        P(None, "row", None, "col", None, None),
        P(None, "row", None, "col"),
        P(None, "col", None, None),
        P(None, "col", None, None),
    )
    return jax.shard_map(
        body,
        mesh=mesh,
        in_specs=placed,
        out_specs=(P(None, "row", None, None), P(None, "row", None, "col", None, None)),
        check_vma=False,
    )
```

```python
import functools

import jax
import jax.numpy as jnp
from jax import lax
from jax.experimental import pallas as pl
from jax.experimental.pallas import tpu as pltpu
from jax.sharding import PartitionSpec as P

MESH = pl.DeviceIdType.MESH
F32 = jnp.float32
BF16 = jnp.bfloat16
CHUNKS = 8


def halves(value):
    high = value.astype(BF16)
    return high, (value - high.astype(F32)).astype(BF16)


def mul(a, b):
    return jnp.dot(a, b, preferred_element_type=F32)


def dot3(left, high, low):
    left_high, left_low = halves(left)
    rows = left.shape[0]
    both = mul(jnp.concatenate([left_high, left_low], axis=0), high)
    return both[:rows] + both[rows:] + mul(left_high, low)


def dot_full(left, right):
    left_high, left_low = halves(left)
    right_high, right_low = halves(right)
    return mul(left_high, right_high) + (mul(left_low, right_high) + mul(left_high, right_low))


def kernel(
    sizes,
    flags,
    wide_hbm,
    narrow_hbm,
    x_ref,
    g_ref,
    rhs_hbm,
    grad_hbm,
    wide,
    narrow,
    l_high,
    l_low,
    below,
    below_two,
    w_full,
    w_high,
    w_low,
    v_high,
    v_low,
    u_high,
    u_low,
    g_turned,
    x_high,
    x_low,
    y_buf,
    chain,
    chain_two,
    part,
    rhs_out,
    grad_out,
    load_sem,
    store_sem,
    below_send,
    below_recv,
    chain_send,
    chain_recv,
    two_send,
    two_recv,
    row_recv,
    x_send,
    y_send,
    part_send,
    part_recv,
):
    n_row, n_col, nx, ny, tile, rhs, chunks = sizes
    n_tiles = 2 * n_row
    width = rhs // chunks
    r = lax.axis_index("row")
    c = lax.axis_index("col")
    x = lax.rem(c, nx)
    y = lax.div(c, nx)
    diag_row = lax.rem(c, n_row)
    diag_slot = lax.div(c, n_row)
    is_diag = r == diag_row
    last_two = n_tiles * 5 // 8
    with_two = c <= last_two
    first = c + jnp.where(with_two, 3, 2)

    loads = [
        pltpu.make_async_copy(wide_hbm.at[s], wide.at[s], load_sem.at[s]) for s in range(2)
    ] + [
        pltpu.make_async_copy(narrow_hbm.at[s], narrow.at[s], load_sem.at[2 + s]) for s in range(2)
    ]
    for load in loads:
        load.start()

    barrier = pltpu.get_barrier_semaphore()

    def greet(row, col):
        pl.semaphore_signal(barrier, inc=1, device_id=(row, col), device_id_type=MESH)

    for d in range(1, nx):
        greet(r, y * nx + lax.rem(x + d, nx))
    for d in range(1, ny):
        greet(r, lax.rem(y + d, ny) * nx + x)
    for d in range(1, n_row):
        greet(lax.rem(r + d, n_row), c)
    peers = nx + ny + n_row - 3

    gives_two = is_diag & (c >= 2) & (c <= last_two + 2)
    takes_two = is_diag & with_two

    @pl.when(is_diag & (c > 0))
    def _():
        greet(lax.rem(c + n_row - 1, n_row), c - 1)

    @pl.when(is_diag & (c < n_tiles - 1))
    def _():
        greet(lax.rem(c + 1, n_row), c + 1)

    @pl.when(gives_two)
    def _():
        greet(lax.rem(c + n_row - 2, n_row), c - 2)

    @pl.when(takes_two)
    def _():
        greet(lax.rem(c + 2, n_row), c + 2)

    links = jnp.where(c > 0, 1, 0) + jnp.where(c < n_tiles - 1, 1, 0)
    links = jnp.where(is_diag, links, 0) + jnp.where(gives_two, 1, 0) + jnp.where(takes_two, 1, 0)
    pl.semaphore_wait(barrier, peers + links)

    for load in loads:
        load.wait()
    step = min(64, tile)
    for s in range(2):
        from_narrow = flags[s] == 1

        def choose(n, _, s=s, from_narrow=from_narrow):
            rows = pl.ds(pl.multiple_of(n * step, step), step)
            value = jnp.where(from_narrow, narrow[s, rows, :].astype(F32), wide[s, rows, :])
            wide[s, rows, :] = value
            high, low = halves(value)
            l_high[s, rows, :] = high
            l_low[s, rows, :] = low
            return 0

        lax.fori_loop(0, tile // step, choose, 0)

    holds_below = (r == lax.rem(c + 1, n_row)) & (c < n_tiles - 1)
    below_slot = jnp.minimum(lax.div(c + 1, n_row), 1)
    below_copy = pltpu.make_async_remote_copy(
        src_ref=wide.at[below_slot],
        dst_ref=below,
        send_sem=below_send.at[0],
        recv_sem=below_recv.at[0],
        device_id=(diag_row, c),
        device_id_type=MESH,
    )

    holds_two = (r == lax.rem(c + 2, n_row)) & with_two
    two_slot = jnp.minimum(lax.div(c + 2, n_row), 1)
    below_two_copy = pltpu.make_async_remote_copy(
        src_ref=wide.at[two_slot],
        dst_ref=below_two,
        send_sem=below_send.at[1],
        recv_sem=below_recv.at[1],
        device_id=(diag_row, c),
        device_id_type=MESH,
    )

    @pl.when(holds_below)
    def _():
        below_copy.start()

    @pl.when(holds_two)
    def _():
        below_two_copy.start()

    turned_x = jnp.transpose(x_ref[...])
    x_high[...], x_low[...] = halves(turned_x)

    half = tile // 2

    def sends_part(row):
        return (row != diag_row) & (row + n_row >= first)

    @pl.when(is_diag)
    def _():
        turned_g = jnp.transpose(g_ref[...])
        for k in range(chunks):
            g_turned[k] = turned_g[k * width : (k + 1) * width]
        for row in range(n_row):

            @pl.when(jnp.logical_not(sends_part(row)))
            def _(row=row):
                part[row] = jnp.zeros(part.shape[1:], F32)

        rows = lax.broadcasted_iota(jnp.int32, (half, half), 0)
        cols = lax.broadcasted_iota(jnp.int32, (half, half), 1)
        for b in range(2):
            w_full[b * half : (b + 1) * half, b * half : (b + 1) * half] = jnp.zeros((half, half), F32)
        blocks = []
        inverses = []
        for b in range(2):
            at = slice(b * half, (b + 1) * half)
            block = wide[diag_slot, at, at]
            on_diag = jnp.where(rows == cols, block, 0.0)
            down = 1.0 / jnp.sum(on_diag, axis=1, keepdims=True)
            across = 1.0 / jnp.sum(on_diag, axis=0, keepdims=True)
            pairs = (rows == cols + 1) & (lax.rem(rows, 2) == 1)
            inverse = jnp.where(rows == cols, down, 0.0) - jnp.where(pairs, block * down * across, 0.0)
            blocks.append(block)
            inverses.append(inverse)
        size = 2
        while size < half:
            mask = (lax.div(rows, 2 * size) == lax.div(cols, 2 * size)) & (
                lax.rem(lax.div(rows, size), 2) > lax.rem(lax.div(cols, size), 2)
            )
            for b in range(2):
                coupling = jnp.where(mask, blocks[b], 0.0)
                product = dot_full(coupling, inverses[b])
                inverses[b] = inverses[b] - dot_full(inverses[b], product)
            size *= 2
        coupling = wide[diag_slot, half:, :half]
        product = dot_full(coupling, inverses[0])
        corner = -dot_full(inverses[1], product)
        w_full[:half, :half] = inverses[0]
        w_full[:half, half:] = jnp.zeros((half, half), F32)
        w_full[half:, :half] = corner
        w_full[half:, half:] = inverses[1]
        high, low = halves(w_full[...])
        w_high[...] = high
        w_low[...] = low

    def fold(source, high_ref, low_ref):
        def some(n, _):
            at = pl.ds(pl.multiple_of(n * (tile // 4), tile // 4), tile // 4)
            high, low = halves(dot3(source[at, :], w_high[...], w_low[...]))
            high_ref[at, :] = high
            low_ref[at, :] = low
            return 0

        lax.fori_loop(0, 4, some, 0)

    def chain_copy(k):
        return pltpu.make_async_remote_copy(
            src_ref=y_buf.at[diag_slot, k],
            dst_ref=chain.at[k],
            send_sem=chain_send.at[k],
            recv_sem=chain_recv.at[k],
            device_id=(lax.rem(c + n_row - 1, n_row), jnp.maximum(c - 1, 0)),
            device_id_type=MESH,
        )

    def two_copy(k):
        return pltpu.make_async_remote_copy(
            src_ref=y_buf.at[diag_slot, k],
            dst_ref=chain_two.at[k],
            send_sem=two_send.at[k],
            recv_sem=two_recv.at[k],
            device_id=(lax.rem(c + n_row - 2, n_row), jnp.maximum(c - 2, 0)),
            device_id_type=MESH,
        )

    def x_copy(s, k):
        return pltpu.make_async_remote_copy(
            src_ref=y_buf.at[s, k],
            dst_ref=y_buf.at[s, k],
            send_sem=x_send.at[s, k],
            recv_sem=row_recv.at[s, k],
            device_id=(r, y * nx + lax.rem(x + 1, nx)),
            device_id_type=MESH,
        )

    def y_copy(s, k, d):
        return pltpu.make_async_remote_copy(
            src_ref=y_buf.at[s, k],
            dst_ref=y_buf.at[s, k],
            send_sem=y_send.at[d, k],
            recv_sem=row_recv.at[s, k],
            device_id=(r, lax.rem(y + d, ny) * nx + x),
            device_id_type=MESH,
        )

    def part_copy(row, k):
        return pltpu.make_async_remote_copy(
            src_ref=part.at[row, k],
            dst_ref=part.at[row, k],
            send_sem=part_send.at[k],
            recv_sem=part_recv.at[row, k],
            device_id=(diag_row, c),
            device_id_type=MESH,
        )

    def roles(s):
        i = r + n_row * s
        takes_part = i >= first
        if s == 1:
            sends_now = takes_part & (r != diag_row) & (r < first)
        else:
            sends_now = takes_part
        passes_on = lax.rem(x + 1, nx) != lax.rem(i, nx)
        return i, takes_part, sends_now, passes_on

    for s in (1, 0):
        i, takes_part, sends_now, passes_on = roles(s)
        is_source = i == c

        @pl.when(is_source)
        def _(s=s):
            @pl.when(c < n_tiles - 1)
            def _():
                below_copy.wait_recv()
                fold(below, v_high, v_low)

            @pl.when(with_two)
            def _():
                below_two_copy.wait_recv()
                fold(below_two, u_high, u_low)

            def solve(k, _):
                for row in range(n_row):

                    @pl.when(sends_part(row))
                    def _(row=row):
                        part_copy(row, k).wait_recv()

                total = g_turned[k]
                for row in range(n_row):
                    total = total - part[row, k]
                y_buf[s, k] = dot3(total, w_high[...], w_low[...])

                @pl.when(with_two)
                def _():
                    two_copy(k).wait_recv()
                    y_buf[s, k] = y_buf[s, k] - dot3(chain_two[k], u_high[...], u_low[...])

                @pl.when(c < n_tiles - 1)
                def _():
                    chain_copy(k).wait_recv()
                    y_buf[s, k] = y_buf[s, k] - dot3(chain[k], v_high[...], v_low[...])

                @pl.when(c > 0)
                def _():
                    chain_copy(k).start()

                for d in range(ny - 1, 0, -1):
                    y_copy(s, k, d).start()

                @pl.when(gives_two)
                def _():
                    two_copy(k).start()

                x_copy(s, k).start()
                return 0

            lax.fori_loop(0, chunks, solve, 0)

        @pl.when(jnp.logical_not(is_source))
        def _(s=s, takes_part=takes_part, sends_now=sends_now, passes_on=passes_on):
            def take(k, _):
                x_copy(s, k).wait_recv()

                @pl.when(passes_on)
                def _():
                    x_copy(s, k).start()

                @pl.when(takes_part)
                def _():
                    product = dot3(y_buf[s, k], l_high[s], l_low[s])
                    if s == 0:
                        product = product + part[r, k]
                    part[r, k] = product

                @pl.when(sends_now)
                def _():
                    part_copy(r, k).start()

                return 0

            lax.fori_loop(0, chunks, take, 0)

        block = jnp.concatenate([y_buf[s, k] for k in range(chunks)], axis=0)
        rhs_out[s] = jnp.transpose(block)
        quarter = tile // 4

        def outer(n, _, s=s, i=i):
            at = pl.ds(pl.multiple_of(n * quarter, quarter), quarter)
            value = -dot3(rhs_out[s, at, :], x_high[...], x_low[...])
            rows = lax.broadcasted_iota(jnp.int32, (quarter, tile), 0) + n * quarter
            cols = lax.broadcasted_iota(jnp.int32, (quarter, tile), 1)
            keep = (rows + i * tile) >= (cols + c * tile)
            grad_out[s, at, :] = jnp.where(keep, value, 0.0)
            return 0

        lax.fori_loop(0, 4, outer, 0)
        pltpu.make_async_copy(rhs_out.at[s], rhs_hbm.at[s], store_sem.at[s]).start()
        pltpu.make_async_copy(grad_out.at[s], grad_hbm.at[s], store_sem.at[2 + s]).start()

    @pl.when(holds_below)
    def _():
        below_copy.wait_send()

    @pl.when(holds_two)
    def _():
        below_two_copy.wait_send()

    for s in (1, 0):
        i, takes_part, sends_now, passes_on = roles(s)

        @pl.when(i == c)
        def _(s=s):
            def ended(k, _):
                @pl.when(c > 0)
                def _():
                    chain_copy(k).wait_send()

                @pl.when(gives_two)
                def _():
                    two_copy(k).wait_send()

                for d in range(1, ny):
                    y_copy(s, k, d).wait_send()
                return 0

            lax.fori_loop(0, chunks, ended, 0)

        @pl.when(passes_on)
        def _(s=s):
            def ended(k, _):
                x_copy(s, k).wait_send()
                return 0

            lax.fori_loop(0, chunks, ended, 0)

        @pl.when((i != c) & sends_now)
        def _():
            def ended(k, _):
                part_copy(r, k).wait_send()
                return 0

            lax.fori_loop(0, chunks, ended, 0)

        pltpu.make_async_copy(rhs_out.at[s], rhs_hbm.at[s], store_sem.at[s]).wait()
        pltpu.make_async_copy(grad_out.at[s], grad_hbm.at[s], store_sem.at[2 + s]).wait()


def solution(mesh):
    n_row, n_col = mesh.shape["row"], mesh.shape["col"]
    nx = 4 if n_col > 4 else 2
    ny = n_col // nx

    def body(factor_wide, factor_narrow, flags, forward_solution, solution_grad):
        slots, _, _, _, tile, _ = factor_wide.shape
        rhs = forward_solution.shape[-1]
        chunks = CHUNKS
        width = rhs // chunks
        sizes = (n_row, n_col, nx, ny, tile, rhs, chunks)
        vmem = pltpu.VMEM
        dma = pltpu.SemaphoreType.DMA
        rhs_grad, factor_grad = pl.pallas_call(
            functools.partial(kernel, sizes),
            out_shape=(
                jax.ShapeDtypeStruct((slots, tile, rhs), F32),
                jax.ShapeDtypeStruct((slots, tile, tile), F32),
            ),
            in_specs=[
                pl.BlockSpec(memory_space=pltpu.SMEM),
                pl.BlockSpec(memory_space=pl.ANY),
                pl.BlockSpec(memory_space=pl.ANY),
                pl.BlockSpec(memory_space=pltpu.VMEM),
                pl.BlockSpec(memory_space=pltpu.VMEM),
            ],
            out_specs=(
                pl.BlockSpec(memory_space=pl.ANY),
                pl.BlockSpec(memory_space=pl.ANY),
            ),
            scratch_shapes=[
                vmem((slots, tile, tile), F32),
                vmem((slots, tile, tile), BF16),
                vmem((slots, tile, tile), BF16),
                vmem((slots, tile, tile), BF16),
                vmem((tile, tile), F32),
                vmem((tile, tile), F32),
                vmem((tile, tile), F32),
                vmem((tile, tile), BF16),
                vmem((tile, tile), BF16),
                vmem((tile, tile), BF16),
                vmem((tile, tile), BF16),
                vmem((tile, tile), BF16),
                vmem((tile, tile), BF16),
                vmem((chunks, width, tile), F32),
                vmem((rhs, tile), BF16),
                vmem((rhs, tile), BF16),
                vmem((slots, chunks, width, tile), F32),
                vmem((chunks, width, tile), F32),
                vmem((chunks, width, tile), F32),
                vmem((n_row, chunks, width, tile), F32),
                vmem((slots, tile, rhs), F32),
                vmem((slots, tile, tile), F32),
                dma((4,)),
                dma((4,)),
                dma((2,)),
                dma((2,)),
                dma((chunks,)),
                dma((chunks,)),
                dma((chunks,)),
                dma((chunks,)),
                dma((slots, chunks)),
                dma((slots, chunks)),
                dma((ny, chunks)),
                dma((chunks,)),
                dma((n_row, chunks)),
            ],
            compiler_params=pltpu.CompilerParams(collective_id=0, has_side_effects=True),
        )(
            flags.reshape(slots),
            factor_wide.reshape(slots, tile, tile),
            factor_narrow.reshape(slots, tile, tile),
            forward_solution.reshape(tile, rhs),
            solution_grad.reshape(tile, rhs),
        )
        return (
            rhs_grad[:, None],
            factor_grad.reshape(slots, 1, 1, 1, tile, tile),
        )

    placed = (
        P(None, "row", None, "col", None, None),
        P(None, "row", None, "col", None, None),
        P(None, "row", None, "col"),
        P(None, "col", None, None),
        P(None, "col", None, None),
    )
    return jax.shard_map(
        body,
        mesh=mesh,
        in_specs=placed,
        out_specs=(P(None, "row", None, None), P(None, "row", None, "col", None, None)),
        check_vma=False,
    )
```

```python
import functools

import jax
import jax.numpy as jnp
from jax import lax
from jax.experimental import pallas as pl
from jax.experimental.pallas import tpu as pltpu
from jax.sharding import PartitionSpec as P

MESH = pl.DeviceIdType.MESH
F32 = jnp.float32
BF16 = jnp.bfloat16
CHUNKS = 8


def halves(value):
    high = value.astype(BF16)
    return high, (value - high.astype(F32)).astype(BF16)


def mul(a, b):
    return jnp.dot(a, b, preferred_element_type=F32)


def dot3(left, high, low):
    left_high, left_low = halves(left)
    rows = left.shape[0]
    both = mul(jnp.concatenate([left_high, left_low], axis=0), high)
    return both[:rows] + both[rows:] + mul(left_high, low)


def dot_full(left, right):
    left_high, left_low = halves(left)
    right_high, right_low = halves(right)
    return mul(left_high, right_high) + (mul(left_low, right_high) + mul(left_high, right_low))


def kernel(
    sizes,
    flags,
    wide_hbm,
    narrow_hbm,
    x_ref,
    g_ref,
    rhs_out,
    grad_out,
    wide,
    narrow,
    l_high,
    l_low,
    below,
    below_two,
    w_full,
    w_high,
    w_low,
    v_high,
    v_low,
    u_high,
    u_low,
    g_turned,
    x_high,
    x_low,
    y_buf,
    chain,
    chain_two,
    part,
    sums,
    totals,
    load_sem,
    below_send,
    below_recv,
    chain_send,
    chain_recv,
    two_send,
    two_recv,
    row_recv,
    x_send,
    y_send,
    part_send,
    sums_recv,
    totals_recv,
):
    n_row, n_col, nx, ny, tile, rhs, chunks = sizes
    n_tiles = 2 * n_row
    width = rhs // chunks
    r = lax.axis_index("row")
    c = lax.axis_index("col")
    x = lax.rem(c, nx)
    y = lax.div(c, nx)
    diag_row = lax.rem(c, n_row)
    diag_slot = lax.div(c, n_row)
    is_diag = r == diag_row
    last_two = n_tiles * 5 // 8
    with_two = c <= last_two
    first = c + jnp.where(with_two, 3, 2)

    loads = [
        pltpu.make_async_copy(wide_hbm.at[s], wide.at[s], load_sem.at[s]) for s in range(2)
    ] + [
        pltpu.make_async_copy(narrow_hbm.at[s], narrow.at[s], load_sem.at[2 + s]) for s in range(2)
    ]
    for load in loads:
        load.start()

    barrier = pltpu.get_barrier_semaphore()

    def greet(row, col):
        pl.semaphore_signal(barrier, inc=1, device_id=(row, col), device_id_type=MESH)

    for d in range(1, nx):
        greet(r, y * nx + lax.rem(x + d, nx))
    for d in range(1, ny):
        greet(r, lax.rem(y + d, ny) * nx + x)
    for d in range(1, n_row):
        greet(lax.rem(r + d, n_row), c)
    peers = nx + ny + n_row - 3

    gives_two = is_diag & (c >= 2) & (c <= last_two + 2)
    takes_two = is_diag & with_two

    @pl.when(is_diag & (c > 0))
    def _():
        greet(lax.rem(c + n_row - 1, n_row), c - 1)

    @pl.when(is_diag & (c < n_tiles - 1))
    def _():
        greet(lax.rem(c + 1, n_row), c + 1)

    @pl.when(gives_two)
    def _():
        greet(lax.rem(c + n_row - 2, n_row), c - 2)

    @pl.when(takes_two)
    def _():
        greet(lax.rem(c + 2, n_row), c + 2)

    links = jnp.where(c > 0, 1, 0) + jnp.where(c < n_tiles - 1, 1, 0)
    links = jnp.where(is_diag, links, 0) + jnp.where(gives_two, 1, 0) + jnp.where(takes_two, 1, 0)
    pl.semaphore_wait(barrier, peers + links)

    for load in loads:
        load.wait()
    step = min(64, tile)
    for s in range(2):
        from_narrow = flags[s] == 1

        def choose(n, _, s=s, from_narrow=from_narrow):
            rows = pl.ds(pl.multiple_of(n * step, step), step)
            value = jnp.where(from_narrow, narrow[s, rows, :].astype(F32), wide[s, rows, :])
            wide[s, rows, :] = value
            high, low = halves(value)
            l_high[s, rows, :] = high
            l_low[s, rows, :] = low
            return 0

        lax.fori_loop(0, tile // step, choose, 0)

    holds_below = (r == lax.rem(c + 1, n_row)) & (c < n_tiles - 1)
    below_slot = jnp.minimum(lax.div(c + 1, n_row), 1)
    below_copy = pltpu.make_async_remote_copy(
        src_ref=wide.at[below_slot],
        dst_ref=below,
        send_sem=below_send.at[0],
        recv_sem=below_recv.at[0],
        device_id=(diag_row, c),
        device_id_type=MESH,
    )

    holds_two = (r == lax.rem(c + 2, n_row)) & with_two
    two_slot = jnp.minimum(lax.div(c + 2, n_row), 1)
    below_two_copy = pltpu.make_async_remote_copy(
        src_ref=wide.at[two_slot],
        dst_ref=below_two,
        send_sem=below_send.at[1],
        recv_sem=below_recv.at[1],
        device_id=(diag_row, c),
        device_id_type=MESH,
    )

    @pl.when(holds_below)
    def _():
        below_copy.start()

    @pl.when(holds_two)
    def _():
        below_two_copy.start()

    turned_x = jnp.transpose(x_ref[...])
    x_high[...], x_low[...] = halves(turned_x)

    half = tile // 2

    @pl.when(is_diag)
    def _():
        turned_g = jnp.transpose(g_ref[...])
        for k in range(chunks):
            g_turned[k] = turned_g[k * width : (k + 1) * width]
        rows = lax.broadcasted_iota(jnp.int32, (half, half), 0)
        cols = lax.broadcasted_iota(jnp.int32, (half, half), 1)
        for b in range(2):
            w_full[b * half : (b + 1) * half, b * half : (b + 1) * half] = jnp.zeros((half, half), F32)
        blocks = []
        inverses = []
        for b in range(2):
            at = slice(b * half, (b + 1) * half)
            block = wide[diag_slot, at, at]
            on_diag = jnp.where(rows == cols, block, 0.0)
            down = 1.0 / jnp.sum(on_diag, axis=1, keepdims=True)
            across = 1.0 / jnp.sum(on_diag, axis=0, keepdims=True)
            pairs = (rows == cols + 1) & (lax.rem(rows, 2) == 1)
            inverse = jnp.where(rows == cols, down, 0.0) - jnp.where(pairs, block * down * across, 0.0)
            blocks.append(block)
            inverses.append(inverse)
        size = 2
        while size < half:
            mask = (lax.div(rows, 2 * size) == lax.div(cols, 2 * size)) & (
                lax.rem(lax.div(rows, size), 2) > lax.rem(lax.div(cols, size), 2)
            )
            for b in range(2):
                coupling = jnp.where(mask, blocks[b], 0.0)
                product = dot_full(coupling, inverses[b])
                inverses[b] = inverses[b] - dot_full(inverses[b], product)
            size *= 2
        coupling = wide[diag_slot, half:, :half]
        product = dot_full(coupling, inverses[0])
        corner = -dot_full(inverses[1], product)
        w_full[:half, :half] = inverses[0]
        w_full[:half, half:] = jnp.zeros((half, half), F32)
        w_full[half:, :half] = corner
        w_full[half:, half:] = inverses[1]
        high, low = halves(w_full[...])
        w_high[...] = high
        w_low[...] = low

    def fold(source, high_ref, low_ref):
        def some(n, _):
            at = pl.ds(pl.multiple_of(n * (tile // 4), tile // 4), tile // 4)
            high, low = halves(dot3(source[at, :], w_high[...], w_low[...]))
            high_ref[at, :] = high
            low_ref[at, :] = low
            return 0

        lax.fori_loop(0, 4, some, 0)

    def chain_copy(k):
        return pltpu.make_async_remote_copy(
            src_ref=y_buf.at[diag_slot, k],
            dst_ref=chain.at[k],
            send_sem=chain_send.at[k],
            recv_sem=chain_recv.at[k],
            device_id=(lax.rem(c + n_row - 1, n_row), jnp.maximum(c - 1, 0)),
            device_id_type=MESH,
        )

    def two_copy(k):
        return pltpu.make_async_remote_copy(
            src_ref=y_buf.at[diag_slot, k],
            dst_ref=chain_two.at[k],
            send_sem=two_send.at[k],
            recv_sem=two_recv.at[k],
            device_id=(lax.rem(c + n_row - 2, n_row), jnp.maximum(c - 2, 0)),
            device_id_type=MESH,
        )

    def x_copy(s, k, d):
        return pltpu.make_async_remote_copy(
            src_ref=y_buf.at[s, k],
            dst_ref=y_buf.at[s, k],
            send_sem=x_send.at[s, d, k],
            recv_sem=row_recv.at[s, k],
            device_id=(r, y * nx + lax.rem(x + d, nx)),
            device_id_type=MESH,
        )

    def y_copy(s, k, d):
        return pltpu.make_async_remote_copy(
            src_ref=y_buf.at[s, k],
            dst_ref=y_buf.at[s, k],
            send_sem=y_send.at[d, k],
            recv_sem=row_recv.at[s, k],
            device_id=(r, lax.rem(y + d, ny) * nx + x),
            device_id_type=MESH,
        )

    def part_copy(s, k, ends):
        if ends:
            dst, sem, row = totals.at[k], totals_recv.at[k], diag_row
        else:
            slot = jnp.where(r > 0, s, max(s - 1, 0))
            dst, sem, row = sums.at[slot, k], sums_recv.at[slot, k], lax.rem(r + n_row - 1, n_row)
        return pltpu.make_async_remote_copy(
            src_ref=part.at[s, k],
            dst_ref=dst,
            send_sem=part_send.at[s, k],
            recv_sem=sem,
            device_id=(row, c),
            device_id_type=MESH,
        )

    def sums_copy(s, k):
        return pltpu.make_async_remote_copy(
            src_ref=part.at[s, k],
            dst_ref=sums.at[s, k],
            send_sem=part_send.at[s, k],
            recv_sem=sums_recv.at[s, k],
            device_id=(lax.rem(r + n_row - 1, n_row), c),
            device_id_type=MESH,
        )

    def place(s):
        i = r + n_row * s
        from_x, from_y = lax.rem(i, nx), lax.div(i, nx)
        serves_line = (x == from_x) & ((y != from_y) | (i == 0))
        passes_on = (y == from_y) & (i > 0) & (lax.rem(x + 1, nx) != from_x)
        return i, i >= first, serves_line, passes_on

    def send_x(s, k, serves_line, passes_on, act):
        @pl.when(serves_line)
        def _():
            for d in range(1, nx):
                act(x_copy(s, k, d))

        @pl.when(passes_on)
        def _():
            act(x_copy(s, k, 1))

    def start(copy):
        copy.start()

    def wait_sent(copy):
        copy.wait_send()

    for s in (1, 0):
        i, takes_part, serves_line, passes_on = place(s)
        is_source = i == c

        @pl.when(is_source)
        def _(s=s, serves_line=serves_line, passes_on=passes_on):
            @pl.when(c < n_tiles - 1)
            def _():
                below_copy.wait_recv()
                fold(below, v_high, v_low)

            @pl.when(with_two)
            def _():
                below_two_copy.wait_recv()
                fold(below_two, u_high, u_low)

            def solve(k, _):
                @pl.when(first < n_tiles)
                def _():
                    part_copy(0, k, True).wait_recv()
                    g_turned[k] = g_turned[k] - totals[k]

                y_buf[s, k] = dot3(g_turned[k], w_high[...], w_low[...])

                @pl.when(with_two)
                def _():
                    two_copy(k).wait_recv()
                    y_buf[s, k] = y_buf[s, k] - dot3(chain_two[k], u_high[...], u_low[...])

                @pl.when(c < n_tiles - 1)
                def _():
                    chain_copy(k).wait_recv()
                    y_buf[s, k] = y_buf[s, k] - dot3(chain[k], v_high[...], v_low[...])

                @pl.when(c > 0)
                def _():
                    chain_copy(k).start()

                for d in range(ny - 1, 0, -1):
                    y_copy(s, k, d).start()

                @pl.when(gives_two)
                def _():
                    two_copy(k).start()

                send_x(s, k, serves_line, passes_on, start)
                return 0

            lax.fori_loop(0, chunks, solve, 0)

        @pl.when(jnp.logical_not(is_source))
        def _(s=s, i=i, takes_part=takes_part, serves_line=serves_line, passes_on=passes_on):
            def take(k, _):
                x_copy(s, k, 1).wait_recv()
                send_x(s, k, serves_line, passes_on, start)

                @pl.when(takes_part)
                def _():
                    part[s, k] = dot3(y_buf[s, k], l_high[s], l_low[s])

                    @pl.when(i < n_tiles - 1)
                    def _():
                        sums_copy(s, k).wait_recv()
                        part[s, k] = part[s, k] + sums[s, k]

                    @pl.when(i > first)
                    def _():
                        part_copy(s, k, False).start()

                    @pl.when(i == first)
                    def _():
                        part_copy(s, k, True).start()

                return 0

            lax.fori_loop(0, chunks, take, 0)

        block = jnp.concatenate([y_buf[s, k] for k in range(chunks)], axis=0)
        rhs_out[s] = jnp.transpose(block)
        quarter = tile // 4

        @pl.when(i < c)
        def _(s=s):
            grad_out[s] = jnp.zeros((tile, tile), F32)

        @pl.when(i >= c)
        def _(s=s, i=i):
            def outer(n, _):
                at = pl.ds(pl.multiple_of(n * quarter, quarter), quarter)
                value = -dot3(rhs_out[s, at, :], x_high[...], x_low[...])
                rows = lax.broadcasted_iota(jnp.int32, (quarter, tile), 0) + n * quarter
                cols = lax.broadcasted_iota(jnp.int32, (quarter, tile), 1)
                keep = (rows + i * tile) >= (cols + c * tile)
                grad_out[s, at, :] = jnp.where(keep, value, 0.0)
                return 0

            lax.fori_loop(0, 4, outer, 0)

    @pl.when(holds_below)
    def _():
        below_copy.wait_send()

    @pl.when(holds_two)
    def _():
        below_two_copy.wait_send()

    for s in (1, 0):
        i, takes_part, serves_line, passes_on = place(s)

        @pl.when(i == c)
        def _(s=s):
            def ended(k, _):
                @pl.when(c > 0)
                def _():
                    chain_copy(k).wait_send()

                @pl.when(gives_two)
                def _():
                    two_copy(k).wait_send()

                for d in range(1, ny):
                    y_copy(s, k, d).wait_send()
                return 0

            lax.fori_loop(0, chunks, ended, 0)

        def ended_line(k, _, s=s, serves_line=serves_line, passes_on=passes_on):
            send_x(s, k, serves_line, passes_on, wait_sent)
            return 0

        lax.fori_loop(0, chunks, ended_line, 0)

        @pl.when((i != c) & takes_part)
        def _(s=s):
            def ended(k, _):
                sums_copy(s, k).wait_send()
                return 0

            lax.fori_loop(0, chunks, ended, 0)


def solution(mesh):
    n_row, n_col = mesh.shape["row"], mesh.shape["col"]
    nx = 4 if n_col > 4 else 2
    ny = n_col // nx

    def body(factor_wide, factor_narrow, flags, forward_solution, solution_grad):
        slots, _, _, _, tile, _ = factor_wide.shape
        rhs = forward_solution.shape[-1]
        chunks = CHUNKS
        width = rhs // chunks
        sizes = (n_row, n_col, nx, ny, tile, rhs, chunks)
        vmem = pltpu.VMEM
        dma = pltpu.SemaphoreType.DMA
        rhs_grad, factor_grad = pl.pallas_call(
            functools.partial(kernel, sizes),
            out_shape=(
                pltpu.VMEM((slots, tile, rhs), F32),
                pltpu.VMEM((slots, tile, tile), F32),
            ),
            in_specs=[
                pl.BlockSpec(memory_space=pltpu.SMEM),
                pl.BlockSpec(memory_space=pl.ANY),
                pl.BlockSpec(memory_space=pl.ANY),
                pl.BlockSpec(memory_space=pltpu.VMEM),
                pl.BlockSpec(memory_space=pltpu.VMEM),
            ],
            out_specs=(
                pl.BlockSpec(memory_space=pltpu.VMEM),
                pl.BlockSpec(memory_space=pltpu.VMEM),
            ),
            scratch_shapes=[
                vmem((slots, tile, tile), F32),
                vmem((slots, tile, tile), BF16),
                vmem((slots, tile, tile), BF16),
                vmem((slots, tile, tile), BF16),
                vmem((tile, tile), F32),
                vmem((tile, tile), F32),
                vmem((tile, tile), F32),
                vmem((tile, tile), BF16),
                vmem((tile, tile), BF16),
                vmem((tile, tile), BF16),
                vmem((tile, tile), BF16),
                vmem((tile, tile), BF16),
                vmem((tile, tile), BF16),
                vmem((chunks, width, tile), F32),
                vmem((rhs, tile), BF16),
                vmem((rhs, tile), BF16),
                vmem((slots, chunks, width, tile), F32),
                vmem((chunks, width, tile), F32),
                vmem((chunks, width, tile), F32),
                vmem((slots, chunks, width, tile), F32),
                vmem((slots, chunks, width, tile), F32),
                vmem((chunks, width, tile), F32),
                dma((4,)),
                dma((2,)),
                dma((2,)),
                dma((chunks,)),
                dma((chunks,)),
                dma((chunks,)),
                dma((chunks,)),
                dma((slots, chunks)),
                dma((slots, nx, chunks)),
                dma((ny, chunks)),
                dma((slots, chunks)),
                dma((slots, chunks)),
                dma((chunks,)),
            ],
            compiler_params=pltpu.CompilerParams(collective_id=0, has_side_effects=True),
        )(
            flags.reshape(slots),
            factor_wide.reshape(slots, tile, tile),
            factor_narrow.reshape(slots, tile, tile),
            forward_solution.reshape(tile, rhs),
            solution_grad.reshape(tile, rhs),
        )
        return (
            rhs_grad[:, None],
            factor_grad.reshape(slots, 1, 1, 1, tile, tile),
        )

    placed = (
        P(None, "row", None, "col", None, None),
        P(None, "row", None, "col", None, None),
        P(None, "row", None, "col"),
        P(None, "col", None, None),
        P(None, "col", None, None),
    )
    return jax.shard_map(
        body,
        mesh=mesh,
        in_specs=placed,
        out_specs=(P(None, "row", None, None), P(None, "row", None, "col", None, None)),
        check_vma=False,
    )
```
